256 devices in a mesh: samp: 32 (over z, x_lo, core), snp: 8 (over x_hi, y).
Axes of the slice: x: 4 (x_hi: 2, x_lo: 2; x = x_hi * 2 + x_lo), y: 4, z: 8, core: 2. Of those that a mesh axis runs over, the one named last changes fastest.
Arguments:
- genotypes: int32 [131072, 4096], P('samp', 'snp'), may hold values from 0 to 2, as said below
- allele_freq: float32 [4096], P('snp'), may hold values from 0.05 to 0.5
- snp_bins: int32 [4096], P('snp'), may hold values from 0 to 11, as said below
- probes: bfloat16 [64, 131072], P(None, 'samp'), may hold values from -6 to 6
- variances: float32 [13], replicated, may hold values from 0.1 to 1
Outputs:
- projected: float32 [131072, 768], P(('samp', 'snp'))
- combined: float32 [64, 131072], P(None, ('samp', 'snp'))
The draws below stay inside these ranges and needn't reach their ends.
Inputs may be any that keep to these rules, and one draw needn't show every extreme that they name: `genotypes`: dosages 0, 1 or 2. `snp_bins`: every component has at least one SNP.
All inputs are finite; a program needn't handle non-finite values.
Results may differ from the reference program's by a relative error of at most 0.0065.
Values may be sent and summed in bfloat16 or wider, within the bound.
No kernel may reach another device: no remote copies, remote signals or barrier semaphores. Data moves between devices by JAX's collectives and lax.ppermute only.
A program may use at most 128 MiB of HBM per device.

```python
import math
import jax
import jax.numpy as jnp
from jax import lax

SNPS = 4096
COMPONENTS = 12
PROBES = 64
ROWS = 4096
SAMPLES = 131072
N_SAMP = 32


def allele_draw(key):
    seeded = jax.random.fold_in(key, 7)
    allele_level = jax.random.randint(jax.random.fold_in(seeded, 1), (SNPS,), 50, 501, dtype=jnp.int32)
    first_copy = jax.random.randint(jax.random.fold_in(seeded, 2), (SAMPLES, SNPS), 0, 1000, dtype=jnp.int32)
    second_copy = jax.random.randint(jax.random.fold_in(seeded, 3), (SAMPLES, SNPS), 0, 1000, dtype=jnp.int32)
    dosage = (first_copy < allele_level[None, :]).astype(jnp.int32) + (second_copy < allele_level[None, :]).astype(jnp.int32)
    return (dosage, allele_level.astype(jnp.float32) / 1000.0)


def draw_genotypes(key, part):
    return allele_draw(key)[0]


def draw_allele_freq(key, part):
    return allele_draw(key)[1]


def draw_snp_bins(key, part):
    seeded = jax.random.fold_in(key, 11)
    places = jax.random.permutation(jax.random.fold_in(seeded, 1), SNPS).astype(jnp.int32)
    first_level = jax.random.randint(jax.random.fold_in(seeded, 2), (SNPS,), 0, COMPONENTS, dtype=jnp.int32)
    second_level = jax.random.randint(jax.random.fold_in(seeded, 3), (SNPS,), 0, COMPONENTS, dtype=jnp.int32)
    skewed = first_level * second_level // (COMPONENTS - 1)
    base_bins = jnp.where(places < COMPONENTS, places, skewed).astype(jnp.int32)
    relabel = jax.random.permutation(jax.random.fold_in(seeded, 4), COMPONENTS).astype(jnp.int32)
    return relabel[base_bins].astype(jnp.int32)


def block_scale(own_key, dims, shards, low, largest):
    def one(position, parts):
        draws = jax.random.uniform(jax.random.fold_in(jax.random.fold_in(own_key, 6), position), (parts,), jnp.float32, low / len(shards), largest / len(shards))
        return jnp.repeat(jnp.exp(draws), dims[position] // parts).reshape((-1,) + (1,) * (len(dims) - position - 1))

    gain = one(*shards[0])
    for cut in shards[1:]:
        gain = gain * one(*cut)
    return gain


def noise(key, dims, scale, limit, shards=(), kind=jnp.bfloat16):
    factor_of = block_scale(key, dims, shards, -0.22, 0.18) if shards else 1.0
    drawn = jax.random.normal(key, dims, jnp.float32) * scale * factor_of
    return jnp.minimum(jnp.maximum(drawn, -limit), limit).astype(kind)


def setup_inputs(seed: int = 0) -> dict:
    keys = jax.random.split(jax.random.key(seed), 6)
    return {
        "genotypes": draw_genotypes(jax.random.fold_in(keys[5], 71), 0),
        "allele_freq": draw_allele_freq(jax.random.fold_in(keys[5], 71), 0),
        "snp_bins": draw_snp_bins(jax.random.fold_in(keys[5], 71), 0),
        "probes": noise(keys[3], (PROBES, SAMPLES), 1.0, 6.0, ((1, 32),)),
        "variances": jnp.clip(jnp.exp(jax.random.uniform(keys[4], (COMPONENTS + 1,), jnp.float32, math.log(0.1), math.log(1.0))), 0.1, 1.0),
    }


def standardize(dosage_block, allele_freq):
    spread = jnp.sqrt(2.0 * allele_freq * (1.0 - allele_freq))
    return ((dosage_block.astype(jnp.float32) - 2.0 * allele_freq) / spread).astype(jnp.bfloat16)

def reference(genotypes, allele_freq, snp_bins, probes, variances):
    dosage_blocks = genotypes.reshape(N_SAMP, ROWS, SNPS)
    probe_blocks = probes.reshape(PROBES, N_SAMP, ROWS).transpose(1, 0, 2)

    def accumulate(carry, pieces):
        dosage_block, probe_block = pieces
        standard = standardize(dosage_block, allele_freq)
        return (carry + jnp.dot(probe_block, standard, preferred_element_type=jnp.float32), None)
    scores, _ = lax.scan(accumulate, jnp.zeros((PROBES, SNPS), jnp.float32), (dosage_blocks, probe_blocks))
    scores = scores / jnp.sqrt(jnp.float32(SAMPLES))
    labels = jnp.arange(COMPONENTS, dtype=jnp.int32)
    onehot = (snp_bins[:, None] == labels[None, :]).astype(jnp.float32)
    counts = lax.optimization_barrier(jnp.sum(onehot, 0))
    factor = lax.optimization_barrier(jnp.sum(onehot * lax.rsqrt(counts)[None, :], 1))
    weights = ((scores.T * factor[:, None])[:, None, :] * onehot[:, :, None]).reshape(SNPS, COMPONENTS * PROBES).astype(jnp.bfloat16)

    def project(dosage_block):
        return jnp.dot(standardize(dosage_block, allele_freq), weights, preferred_element_type=jnp.float32)
    projected = lax.map(project, dosage_blocks).reshape(SAMPLES, COMPONENTS * PROBES)
    stacked = projected.reshape(SAMPLES, COMPONENTS, PROBES)
    combined = jnp.einsum('nmb,m->bn', stacked, variances[:COMPONENTS]) + variances[COMPONENTS] * probes.astype(jnp.float32)
    return (projected, combined)
```

```python
import math

import jax
import jax.numpy as jnp
from jax import lax
from jax.experimental import pallas as pl
from jax.experimental.pallas import tpu as pltpu
from jax.sharding import PartitionSpec as P


COMPONENTS = 12
RING = 4
CORES = 2
SHIFTS = ((1, 0), (0, 1), (0, 3), (1, 1), (1, 3), (0, 2), (1, 2), (0, 0))
STAGES = ((7, 0, 1, 2, 3), (4, 5), (6,))


def standardize_kernel(order_ref, dosage_ref, freq_ref, probes_ref, *outs):
    slots, partial_ref = outs[:-1], outs[-1]
    step = pl.program_id(0)
    freq = freq_ref[...]
    scale = 1.0 / jnp.sqrt(2.0 * freq * (1.0 - freq))
    standard = ((dosage_ref[...].astype(jnp.float32) - 2.0 * freq) * scale).astype(jnp.bfloat16)
    for place, slot in enumerate(slots):

        @pl.when(step == place)
        def _():
            slot[...] = standard

    scores = jnp.dot(probes_ref[...], standard, preferred_element_type=jnp.float32)

    @pl.when(step == 0)
    def _():
        partial_ref[...] = scores

    @pl.when(step > 0)
    def _():
        partial_ref[...] += scores


def standardize_and_score(order, genotypes, allele_freq, probes):
    rows, snps = genotypes.shape
    width = probes.shape[0]
    groups = order.shape[0]
    block = rows // groups
    return pl.pallas_call(
        standardize_kernel,
        grid_spec=pltpu.PrefetchScalarGridSpec(
            num_scalar_prefetch=1,
            grid=(groups,),
            in_specs=[
                pl.BlockSpec((block, snps), lambda i, order: (order[i], 0)),
                pl.BlockSpec((1, snps), lambda i, order: (0, 0)),
                pl.BlockSpec((width, block), lambda i, order: (0, order[i])),
            ],
            out_specs=[pl.BlockSpec((block, snps), lambda i, order: (0, 0))] * groups
            + [pl.BlockSpec((width, snps), lambda i, order: (0, 0))],
        ),
        out_shape=[jax.ShapeDtypeStruct((block, snps), jnp.bfloat16)] * groups
        + [jax.ShapeDtypeStruct((width, snps), jnp.float32)],
    )(order, genotypes, allele_freq[None, :], probes)


def project_kernel(slots, first, last, *refs):
    order_ref, scores_ref, kinds_ref, variances_ref, probes_ref = refs[:5]
    chunk_refs = refs[5 : 5 + len(slots)]
    rest = refs[5 + len(slots) :]
    so_far_ref = None if first else rest[0]
    projected_ref = rest[0 if first else 1]
    kinds_scratch = rest[-1]
    factor_scratch = rest[-2]
    width = scores_ref.shape[1]

    kinds = kinds_ref[...].astype(jnp.float32)
    factor = jnp.zeros_like(kinds)
    for m in range(COMPONENTS):
        hits = kinds == float(m)
        count = jnp.sum(jnp.sum(hits.astype(jnp.float32), 1, keepdims=True), 0, keepdims=True)
        factor = jnp.where(hits, lax.rsqrt(count), factor)
    kinds_scratch[...] = kinds
    factor_scratch[...] = factor

    total = None if first else so_far_ref[...]
    for slot, chunk_ref in zip(slots, chunk_refs):
        source = order_ref[slot]
        kind = kinds_scratch[pl.ds(source, 1), :]
        weighted = scores_ref[source].astype(jnp.float32) * factor_scratch[pl.ds(source, 1), :]
        weights = jnp.concatenate(
            [jnp.where(kind == float(m), weighted, 0.0).astype(jnp.bfloat16) for m in range(COMPONENTS)], 0
        )
        product = lax.dot_general(
            chunk_ref[...], weights, (((1,), (1,)), ((), ())), preferred_element_type=jnp.float32
        )
        total = product if total is None else total + product
    projected_ref[...] = total
    if last:
        mixed = sum(variances_ref[m] * total[:, m * width : (m + 1) * width] for m in range(COMPONENTS))
        rest[2][...] = mixed.T + variances_ref[COMPONENTS] * probes_ref[...].astype(jnp.float32)


def project(stage, order, scores, kinds, variances, own_probes, chunks, so_far):
    slots = STAGES[stage]
    first, last = stage == 0, stage == len(STAGES) - 1
    width, rows = own_probes.shape
    columns = COMPONENTS * width
    whole = pl.BlockSpec(memory_space=pltpu.VMEM)
    scalars = pl.BlockSpec(memory_space=pltpu.SMEM)
    extra = [] if first else [so_far]
    out_shape = [jax.ShapeDtypeStruct((rows, columns), jnp.float32)]
    if last:
        out_shape.append(jax.ShapeDtypeStruct((width, rows), jnp.float32))
    return pl.pallas_call(
        lambda *refs: project_kernel(slots, first, last, *refs),
        in_specs=[scalars, whole, whole, scalars, whole] + [whole] * (len(slots) + len(extra)),
        out_specs=[whole] * len(out_shape),
        out_shape=out_shape,
        scratch_shapes=[pltpu.VMEM(kinds.shape, jnp.float32)] * 2,
    )(order, scores, kinds, variances, own_probes, *[chunks[slot] for slot in slots], *extra)


def exchange(value, axis, target_of):
    return lax.ppermute(value, axis, [(i, target_of(i)) for i in range(lax.axis_size(axis))])


def shifted(index, dx, dy):
    return (index // RING ^ dx) * RING + (index % RING + dy) % RING


def body(genotypes, allele_freq, snp_bins, probes, variances):
    samp, snp = lax.axis_size("samp"), lax.axis_size("snp")
    rows, snps = genotypes.shape
    width = probes.shape[0]
    own_rows = rows // snp
    half = width // CORES
    depth = samp // (2 * CORES)
    core = lax.axis_index("samp") % CORES
    me = lax.axis_index("snp")

    targets = jnp.stack([shifted(me, dx, dy) for dx, dy in SHIFTS]).astype(jnp.int32)
    sources = jnp.stack([shifted(me, dx, RING - dy) for dx, dy in SHIFTS]).astype(jnp.int32)
    *blocks, partial = standardize_and_score(targets, genotypes, allele_freq, probes)
    chunks = [blocks[-1]] * len(SHIFTS)
    for slot, (dx, dy) in enumerate(SHIFTS[:-1]):
        chunks[slot] = exchange(blocks[slot], "snp", lambda i: shifted(i, dx, dy))

    halves = (partial * (1.0 / math.sqrt(rows * samp))).reshape(CORES, half, snps)
    other = exchange(lax.dynamic_index_in_dim(halves, 1 - core, 0, keepdims=False), "samp", lambda i: i ^ 1)
    mine = lax.dynamic_index_in_dim(halves, core, 0, keepdims=False) + other
    flip = 1
    while flip < depth:
        mine = mine + exchange(mine, "samp", lambda i: i ^ (2 * CORES * flip))
        flip *= 2

    tail = jnp.zeros((half, snps // 4), jnp.bfloat16).at[:4].set(snp_bins.astype(jnp.bfloat16).reshape(4, snps // 4))
    packed = jnp.concatenate([mine.astype(jnp.bfloat16), tail], 1)
    planes = [
        [(z * 2 * CORES + lo * CORES + c) * snp + k for lo in range(2) for k in range(snp)]
        for z in range(depth)
        for c in range(CORES)
    ]
    copies = jnp.broadcast_to(packed, (2 * snp, *packed.shape))
    gathered = lax.all_to_all(
        copies, ("samp", "snp"), split_axis=0, concat_axis=0, tiled=True, axis_index_groups=planes
    )
    kinds = gathered[:snp, :4, snps:].reshape(snp, snps)
    mine = (gathered[:snp, :, :snps].astype(jnp.float32) + gathered[snp:, :, :snps].astype(jnp.float32)).astype(jnp.bfloat16)
    other = exchange(mine, "samp", lambda i: i ^ 1)
    scores = jnp.concatenate([jnp.where(core == 0, mine, other), jnp.where(core == 0, other, mine)], 1)

    own_probes = lax.dynamic_slice_in_dim(probes, me * own_rows, own_rows, 1)
    state = [None]
    for stage in range(len(STAGES)):
        state = project(stage, sources, scores, kinds, variances, own_probes, chunks, state[0])
    return tuple(state)


def solution(mesh):
    placed = (P("samp", "snp"), P("snp"), P("snp"), P(None, "samp"), P())
    return jax.shard_map(
        body,
        mesh=mesh,
        in_specs=placed,
        out_specs=(P(("samp", "snp"), None), P(None, ("samp", "snp"))),
        check_vma=False,
    )
```
